32 devices in a mesh: row: 4 (over z), col: 8 (over y, x, core).
Axes of the slice: x: 2, y: 2, z: 4, core: 2. Of those that a mesh axis runs over, the one named last changes fastest.
Arguments:
- tokens_in: bfloat16 [8192, 1408], P(('row', 'col')), may hold values from -300 to 300
- ln1_gain: bfloat16 [1408], replicated, may hold values from 0.099609375 to 1.8984375
- ln1_bias: bfloat16 [1408], replicated, may hold values from -3 to 3
- qkv_weight: bfloat16 [1408, 4224], P('row', 'col'), may hold values from -0.8 to 0.8
- qkv_bias: bfloat16 [4224], P('col'), may hold values from -3 to 3
- proj_weight: bfloat16 [1408, 1408], P('col', 'row'), may hold values from -0.15625 to 0.15625
- proj_bias: bfloat16 [1408], replicated, may hold values from -3 to 3
- ln2_gain: bfloat16 [1408], replicated, may hold values from 0.099609375 to 1.8984375
- ln2_bias: bfloat16 [1408], replicated, may hold values from -3 to 3
- fc1_weight: bfloat16 [1408, 6144], P('row', 'col'), may hold values from -0.15625 to 0.15625
- fc1_bias: bfloat16 [6144], P('col'), may hold values from -3 to 3
- fc2_weight: bfloat16 [1408, 6144], P('row', 'col'), may hold values from -0.078125 to 0.078125
- fc2_bias: bfloat16 [1408], replicated, may hold values from -3 to 3
Outputs:
- tokens_out: bfloat16 [8192, 1408], P(('row', 'col'))
The draws below stay inside these ranges and needn't reach their ends.
All inputs are finite; a program needn't handle non-finite values.
Results may differ from the reference program's by a relative error of at most 0.01.
Values may be sent and summed in bfloat16 or wider, within the bound.
A program may use at most 64 MiB of HBM per device.

```python
import jax
import jax.numpy as jnp
from jax import lax

D = 1408
HEADS = 16
FF = 6144
LEN = 2048
TOKENS = 8192
N_ROW = 4
N_COL = 8


def draw_tokens_in(key, part):
    key_base = jax.random.fold_in(key, 11)
    columns = 1.0 + 2.0 * jnp.arange(D, dtype=jnp.float32) / (D - 1)
    base = jax.random.normal(key_base, (TOKENS, D), jnp.float32)
    return (base * columns).astype(jnp.bfloat16)


def draw_qkv_weight(key, part):
    noise = jax.random.normal(jax.random.fold_in(key, 21), (D, 3 * D), jnp.float32) * D ** (-0.5)
    return jnp.clip(noise, -0.8, 0.8).astype(jnp.bfloat16)


def shard_levels(stream_key, dims, cuts, low, largest):
    level, own = 1.0, jax.random.fold_in(stream_key, 6)
    for position, shards_of in cuts:
        draws = jnp.exp(jax.random.uniform(jax.random.fold_in(own, position), (shards_of,), jnp.float32, low / len(cuts), largest / len(cuts)))
        level = level * jnp.repeat(draws, dims[position] // shards_of).reshape([-1 if axis == position else 1 for axis in range(len(dims))])
    return level


def normal_values(own_key, dims, spread, reach, pieces=(), held_as=jnp.bfloat16):
    level = shard_levels(own_key, dims, pieces, -0.22, 0.18) if pieces else 1.0
    drawn = jax.random.normal(own_key, dims, jnp.float32) * spread * level
    return jnp.minimum(jnp.maximum(drawn, -reach), reach).astype(held_as)


def setup_inputs(seed: int = 0) -> dict:
    streams_of = jax.random.split(jax.random.key(seed), 14)
    return {
        "tokens_in": draw_tokens_in(jax.random.fold_in(streams_of[13], 71), 0),
        "ln1_gain": jnp.clip(1.0 + 0.18 * jax.random.normal(streams_of[1], (D,), jnp.float32), 0.099609375, 1.8984375).astype(jnp.bfloat16),
        "ln1_bias": normal_values(streams_of[2], (D,), 0.5, 3.0),
        "qkv_weight": draw_qkv_weight(jax.random.fold_in(streams_of[13], 71), 0),
        "qkv_bias": normal_values(streams_of[4], (3 * D,), 0.5, 3.0, ((0, 8),)),
        "proj_weight": normal_values(streams_of[5], (D, D), D ** -0.5, 0.15625, ((0, 8), (1, 4))),
        "proj_bias": normal_values(streams_of[6], (D,), 0.5, 3.0),
        "ln2_gain": jnp.clip(1.0 + 0.18 * jax.random.normal(streams_of[7], (D,), jnp.float32), 0.099609375, 1.8984375).astype(jnp.bfloat16),
        "ln2_bias": normal_values(streams_of[8], (D,), 0.5, 3.0),
        "fc1_weight": normal_values(streams_of[9], (D, FF), D ** -0.5, 0.15625, ((0, 4), (1, 8))),
        "fc1_bias": normal_values(streams_of[10], (FF,), 0.5, 3.0, ((0, 8),)),
        "fc2_weight": normal_values(streams_of[11], (D, FF), FF ** -0.5, 0.078125, ((0, 4), (1, 8))),
        "fc2_bias": normal_values(streams_of[12], (D,), 0.5, 3.0),
    }


def layer_norm(values, gain, bias):
    mean = lax.optimization_barrier(jnp.mean(values, axis=-1, keepdims=True))
    centred = values - mean
    var = lax.optimization_barrier(jnp.mean(centred * centred, axis=-1, keepdims=True))
    return centred * lax.rsqrt(var + 1e-06) * gain.astype(jnp.float32) + bias.astype(jnp.float32)

def attend(qkv, heads):
    length = qkv.shape[0]
    head_size = qkv.shape[1] // (3 * heads)
    parts = qkv.reshape(length, heads, 3, head_size).astype(jnp.float32)
    query = parts[:, :, 0]
    keys = parts[:, :, 1]
    values = parts[:, :, 2]
    block = min(512, length)
    blocks = query.reshape(length // block, block, heads, head_size)
    scale = 1.0 / head_size ** 0.5

    def one_block(qblock):
        scores = jnp.einsum('qhe,khe->hqk', qblock, keys) * scale
        top = lax.optimization_barrier(jnp.max(scores, axis=-1, keepdims=True))
        expo = jnp.exp(scores - top)
        probs = (expo / lax.optimization_barrier(jnp.sum(expo, axis=-1, keepdims=True))).astype(jnp.bfloat16)
        mixed = jnp.einsum('hqk,khe->qhe', probs.astype(jnp.float32), values)
        return mixed.astype(jnp.bfloat16).reshape(block, heads * head_size)
    return lax.map(one_block, blocks).reshape(length, heads * head_size)

def grouped_sum(left, right, groups):
    width = left.shape[1] // groups
    lefts = left.reshape(left.shape[0], groups, width).transpose(1, 0, 2)
    rights = right.reshape(groups, width, right.shape[1])

    def add_group(total, pair):
        part = jnp.dot(pair[0], pair[1], preferred_element_type=jnp.float32).astype(jnp.bfloat16)
        part = lax.optimization_barrier(part)
        return (total + part.astype(jnp.float32), None)
    start = jnp.zeros((left.shape[0], right.shape[1]), jnp.float32)
    total, _ = lax.scan(add_group, start, (lefts, rights))
    return total

def reference(tokens_in, ln1_gain, ln1_bias, qkv_weight, qkv_bias, proj_weight, proj_bias, ln2_gain, ln2_bias, fc1_weight, fc1_bias, fc2_weight, fc2_bias):
    inputs = tokens_in.astype(jnp.float32)
    ln1 = layer_norm(inputs, ln1_gain, ln1_bias).astype(jnp.bfloat16)
    qkv = jnp.dot(ln1, qkv_weight, preferred_element_type=jnp.float32) + qkv_bias.astype(jnp.float32)
    qkv = qkv.astype(jnp.bfloat16)
    clips = qkv.reshape(N_ROW, LEN, 3 * D)
    attn = lax.map(lambda clip: attend(clip, HEADS), clips).reshape(TOKENS, D)
    resid = inputs + grouped_sum(attn, proj_weight, N_COL) + proj_bias.astype(jnp.float32)
    ln2 = layer_norm(resid, ln2_gain, ln2_bias).astype(jnp.bfloat16)
    hidden = jnp.dot(ln2, fc1_weight, preferred_element_type=jnp.float32) + fc1_bias.astype(jnp.float32)
    hidden = jax.nn.gelu(hidden, approximate=False).astype(jnp.bfloat16)
    result = resid + grouped_sum(hidden, fc2_weight.T, N_COL) + fc2_bias.astype(jnp.float32)
    return result.astype(jnp.bfloat16)
```

```python
import functools

import jax
import jax.numpy as jnp
from jax import lax
from jax.experimental import pallas as pl
from jax.experimental.pallas import tpu as pltpu
from jax.sharding import PartitionSpec as P

HEADS = 16
LANES = 128
MESH = pl.DeviceIdType.MESH


def greet(peers):
    barrier = pltpu.get_barrier_semaphore()
    for peer in peers:
        pl.semaphore_signal(barrier, inc=1, device_id={"col": peer}, device_id_type=MESH)
    pl.semaphore_wait(barrier, len(peers))


def neighbours():
    me = lax.axis_index("col")
    core, x, y = me % 2, (me // 2) % 2, me // 4
    place = lambda y, x, core: y * 4 + x * 2 + core
    return (
        me,
        place(y, x, 1 - core),
        place(y, 1 - x, core),
        place(1 - y, x, core),
        place(1 - y, 1 - x, core),
    )


def gather_kernel(x_ref, o_ref, send, recv, local_sem):
    rows = x_ref.shape[0]
    half = rows // 2
    me, mate, xn, yn, dn = neighbours()
    greet((mate, xn, yn))

    def part(block, h):
        return o_ref.at[pl.ds(pl.multiple_of(block * rows + h * half, half), half)]

    def copy(i, src, block, h, to):
        return pltpu.make_async_remote_copy(
            src_ref=src, dst_ref=part(block, h), send_sem=send.at[i], recv_sem=recv.at[i],
            device_id={"col": to}, device_id_type=MESH,
        )

    def own(h):
        return x_ref.at[pl.ds(h * half, half)]

    def arrived(i, block, h):
        copy(i, own(0), block, h, mate).wait_recv()

    started = []

    def go(c):
        c.start()
        started.append(c)

    go(copy(0, own(0), me, 0, xn))
    go(copy(1, own(1), me, 1, yn))
    go(copy(2, own(1), me, 1, xn))
    go(copy(3, own(0), me, 0, yn))
    go(copy(6, own(0), me, 0, mate))
    go(copy(7, own(1), me, 1, mate))
    here = pltpu.make_async_copy(
        x_ref, o_ref.at[pl.ds(pl.multiple_of(me * rows, rows), rows)], local_sem
    )
    here.start()
    arrived(0, xn, 0)
    go(copy(4, part(xn, 0), xn, 0, yn))
    go(copy(8, part(xn, 0), xn, 0, mate))
    arrived(1, yn, 1)
    go(copy(5, part(yn, 1), yn, 1, xn))
    go(copy(9, part(yn, 1), yn, 1, mate))
    arrived(2, xn, 1)
    go(copy(10, part(xn, 1), xn, 1, mate))
    arrived(3, yn, 0)
    go(copy(11, part(yn, 0), yn, 0, mate))
    arrived(4, dn, 0)
    go(copy(12, part(dn, 0), dn, 0, mate))
    arrived(5, dn, 1)
    go(copy(13, part(dn, 1), dn, 1, mate))
    across = lambda block: block + mate - me
    for i, block, h in (
        (6, me, 0), (7, me, 1), (8, xn, 0), (9, yn, 1),
        (10, xn, 1), (11, yn, 0), (12, dn, 0), (13, dn, 1),
    ):
        arrived(i, across(block), h)
    for c in started:
        c.wait_send()
    here.wait()


def gather_col(x, collective_id):
    n = lax.axis_size("col")
    rows, width = x.shape
    if n != 8 or rows % 32:
        return lax.all_gather(x, "col", axis=0, tiled=True)
    return pl.pallas_call(
        gather_kernel,
        out_shape=jax.ShapeDtypeStruct((n * rows, width), x.dtype),
        in_specs=[pl.BlockSpec(memory_space=pltpu.VMEM)],
        out_specs=pl.BlockSpec(memory_space=pltpu.VMEM),
        scratch_shapes=[
            pltpu.SemaphoreType.DMA((14,)),
            pltpu.SemaphoreType.DMA((14,)),
            pltpu.SemaphoreType.DMA,
        ],
        compiler_params=pltpu.CompilerParams(
            collective_id=collective_id, has_side_effects=True, vmem_limit_bytes=24 << 20
        ),
        cost_estimate=pl.CostEstimate(
            flops=10**10, bytes_accessed=2 * n * rows * width, transcendentals=0
        ),
        name="gather_col",
    )(x)


def scatter_kernel(x_ref, o_ref, mated, sums, relay, landed, send, recv):
    rows = o_ref.shape[0]
    half = rows // 2
    me, mate, xn, yn, dn = neighbours()
    greet((mate, xn, yn))
    shift = mate - me
    targets = (dn, xn, yn, me)

    def copy(i, src, dst, to):
        return pltpu.make_async_remote_copy(
            src_ref=src, dst_ref=dst, send_sem=send.at[i], recv_sem=recv.at[i],
            device_id={"col": to}, device_id_type=MESH,
        )

    def block(j):
        return pl.ds(pl.multiple_of(j * rows, rows), rows)

    started = []

    def go(c):
        c.start()
        started.append(c)

    for k, target in enumerate(targets):
        go(copy(k, x_ref.at[block(target + shift)], mated.at[k], mate))

    def mine(k, h):
        rows_h = pl.ds(pl.multiple_of(targets[k] * rows + h * half, half), half)
        return x_ref[rows_h, :].astype(jnp.float32) + mated[k, pl.ds(h * half, half), :].astype(
            jnp.float32
        )

    def put(k, h, value):
        sums[k, pl.ds(h * half, half), :] = value.astype(jnp.bfloat16)

    def of(ref, k, h):
        return ref.at[k, pl.ds(h * half, half)]

    started[0].wait_recv()
    put(0, 0, mine(0, 0))
    go(copy(4, of(sums, 0, 0), relay.at[0], xn))
    put(0, 1, mine(0, 1))
    go(copy(5, of(sums, 0, 1), relay.at[1], yn))
    started[1].wait_recv()
    put(1, 0, mine(1, 0))
    go(copy(6, of(sums, 1, 0), of(landed, 0, 0), xn))
    started[2].wait_recv()
    put(2, 1, mine(2, 1))
    go(copy(7, of(sums, 2, 1), of(landed, 1, 1), yn))
    started[4].wait_recv()
    put(2, 0, mine(2, 0) + relay[0].astype(jnp.float32))
    go(copy(8, of(sums, 2, 0), of(landed, 1, 0), yn))
    started[5].wait_recv()
    put(1, 1, mine(1, 1) + relay[1].astype(jnp.float32))
    go(copy(9, of(sums, 1, 1), of(landed, 0, 1), xn))
    started[3].wait_recv()
    for i in (6, 7, 8, 9):
        started[i].wait_recv()
    for h in (0, 1):
        lines = pl.ds(h * half, half)
        o_ref[lines, :] = (
            mine(3, h)
            + landed[0, lines, :].astype(jnp.float32)
            + landed[1, lines, :].astype(jnp.float32)
        )
    for c in started:
        c.wait_send()


def scatter_col(x, collective_id):
    n = lax.axis_size("col")
    rows, width = x.shape[0] // n, x.shape[1]
    if n != 8 or rows % 32:
        return lax.psum_scatter(x, "col", scatter_dimension=0, tiled=True).astype(jnp.float32)
    return pl.pallas_call(
        scatter_kernel,
        out_shape=jax.ShapeDtypeStruct((rows, width), jnp.float32),
        in_specs=[pl.BlockSpec(memory_space=pltpu.VMEM)],
        out_specs=pl.BlockSpec(memory_space=pltpu.VMEM),
        scratch_shapes=[
            pltpu.VMEM((4, rows, width), x.dtype),
            pltpu.VMEM((3, rows, width), x.dtype),
            pltpu.VMEM((2, rows // 2, width), x.dtype),
            pltpu.VMEM((2, rows, width), x.dtype),
            pltpu.SemaphoreType.DMA((10,)),
            pltpu.SemaphoreType.DMA((10,)),
        ],
        compiler_params=pltpu.CompilerParams(
            collective_id=collective_id, has_side_effects=True, vmem_limit_bytes=32 << 20
        ),
        cost_estimate=pl.CostEstimate(
            flops=10**10, bytes_accessed=2 * n * rows * width, transcendentals=0
        ),
        name="scatter_col",
    )(x)


def gather_row(weight, axis):
    n = lax.axis_size("row")
    me = lax.axis_index("row")
    depth = weight.shape[axis]
    shape = list(weight.shape)
    shape[axis] *= n
    whole = jnp.zeros(shape, weight.dtype)
    for step in range(n):
        block = weight
        if step:
            block = lax.ppermute(weight, "row", [((i + step) % n, i) for i in range(n)])
        whole = lax.dynamic_update_slice_in_dim(whole, block, ((me + step) % n) * depth, axis)
    return whole


def cube_gather_col(x):
    n = lax.axis_size("col")
    if n != 8:
        return lax.all_gather(x, "col", axis=0, tiled=True)
    me = lax.axis_index("col")
    x = x[None]
    for bit, after in ((2, 1), (4, 2), (1, 4)):
        other = lax.ppermute(x, "col", [(i, i ^ bit) for i in range(n)])
        low = (me // bit) % 2 == 0
        first, second = jnp.where(low, x, other), jnp.where(low, other, x)
        x = jnp.concatenate([first, second], axis=0) if bit != 1 else jnp.stack([first, second], 1)
    return x.reshape(-1, x.shape[-1])


def norm_local(values, gain, bias):
    mean = jnp.mean(values, axis=-1, keepdims=True)
    centred = values - mean
    var = jnp.mean(centred * centred, axis=-1, keepdims=True)
    return centred * lax.rsqrt(var + 1e-06) * gain.astype(jnp.float32) + bias.astype(jnp.float32)


def attend_kernel(heads, size, padded, q_ref, kv_ref, o_ref):
    outs = []
    for head in range(heads):
        base = head * 3 * padded
        query = q_ref[:, base : base + padded]
        keys = kv_ref[:, base + padded : base + 2 * padded]
        values = kv_ref[:, base + 2 * padded : base + 3 * padded]
        scores = lax.dot_general(
            query, keys, (((1,), (1,)), ((), ())), preferred_element_type=jnp.float32
        )
        top = jnp.max(scores, axis=-1, keepdims=True)
        expo = jnp.exp2(scores - top).astype(jnp.bfloat16)
        mixed = jnp.dot(expo, values, preferred_element_type=jnp.float32)
        outs.append(mixed[:, :size] / mixed[:, size : size + 1])
    o_ref[...] = jnp.concatenate(outs, axis=1).astype(o_ref.dtype)


def attend(qkv, heads, size, padded):
    length, width = qkv.shape
    block = min(256, length)
    return pl.pallas_call(
        functools.partial(attend_kernel, heads, size, padded),
        grid=(length // block,),
        in_specs=[
            pl.BlockSpec((block, width), lambda i: (i, 0)),
            pl.BlockSpec((length, width), lambda i: (0, 0)),
        ],
        out_specs=pl.BlockSpec((block, heads * size), lambda i: (i, 0)),
        out_shape=jax.ShapeDtypeStruct((length, heads * size), jnp.bfloat16),
        compiler_params=pltpu.CompilerParams(vmem_limit_bytes=40 << 20),
        cost_estimate=pl.CostEstimate(
            flops=4 * heads * length * length * padded * 8,
            bytes_accessed=4 * length * width,
            transcendentals=heads * length * length,
        ),
        name="attend",
    )(qkv, qkv)


def project_back(left, right):
    return lax.dot_general(
        left, right, (((1,), (1,)), ((), ())), preferred_element_type=jnp.float32
    )


def local(
    tokens_in,
    ln1_gain,
    ln1_bias,
    qkv_weight,
    qkv_bias,
    proj_weight,
    proj_bias,
    ln2_gain,
    ln2_bias,
    fc1_weight,
    fc1_bias,
    fc2_weight,
    fc2_bias,
):
    local_heads = HEADS // lax.axis_size("col")
    own_rows, features = tokens_in.shape
    size = qkv_weight.shape[1] // (3 * local_heads)
    padded = -(-(size + 1) // LANES) * LANES
    inputs = tokens_in.astype(jnp.float32)
    qkv_full = gather_row(qkv_weight, 0)
    proj_full = gather_row(proj_weight, 1)
    fc1_full = gather_row(fc1_weight, 0)
    fc2_full = gather_row(fc2_weight, 0)
    fc1_shift = fc1_bias.astype(jnp.float32)

    spare = padded - size
    qkv_wide = jnp.pad(
        qkv_full.reshape(features, local_heads, 3, size), ((0, 0), (0, 0), (0, 0), (0, spare))
    ).reshape(features, local_heads * 3 * padded)
    shift = jnp.pad(
        qkv_bias.astype(jnp.float32).reshape(local_heads, 3, size), ((0, 0), (0, 0), (0, spare))
    )
    shift = shift.at[:, 2, size].set(1.0).reshape(-1)
    scale = jnp.ones((local_heads, 3, padded), jnp.float32)
    scale = scale.at[:, 0].set(1.4426950408889634 / size**0.5).reshape(-1)

    ln1 = norm_local(inputs, ln1_gain, ln1_bias).astype(jnp.bfloat16)
    product = jnp.dot(gather_col(ln1, 0), qkv_wide, preferred_element_type=jnp.float32)
    qkv = ((product + shift) * scale).astype(jnp.bfloat16)
    attn = attend(qkv, local_heads, size, padded)
    proj_whole = cube_gather_col(proj_full)
    own_heads = lax.all_to_all(attn, "col", split_axis=0, concat_axis=1, tiled=True)
    attn_sum = jnp.dot(own_heads, proj_whole, preferred_element_type=jnp.float32)
    resid = inputs + attn_sum + proj_bias.astype(jnp.float32)
    ln2 = norm_local(resid, ln2_gain, ln2_bias).astype(jnp.bfloat16)
    product = jnp.dot(gather_col(ln2, 1), fc1_full, preferred_element_type=jnp.float32) + fc1_shift
    hidden = jax.nn.gelu(product, approximate=False).astype(jnp.bfloat16)
    mlp_sum = scatter_col(project_back(hidden, fc2_full).astype(jnp.bfloat16), 2)
    result = resid + mlp_sum + fc2_bias.astype(jnp.float32)
    return result.astype(jnp.bfloat16)


def solution(mesh):
    in_specs = (
        P(("row", "col"), None),
        P(),
        P(),
        P("row", "col"),
        P("col"),
        P("col", "row"),
        P(),
        P(),
        P(),
        P("row", "col"),
        P("col"),
        P("row", "col"),
        P(),
    )
    out_specs = P(("row", "col"), None)
    return jax.shard_map(local, mesh=mesh, in_specs=in_specs, out_specs=out_specs, check_vma=False)
```

```python
import functools

import jax
import jax.numpy as jnp
from jax import lax
from jax.experimental import pallas as pl
from jax.experimental.pallas import tpu as pltpu
from jax.sharding import PartitionSpec as P

HEADS = 16
LANES = 128
MESH = pl.DeviceIdType.MESH


def greet(peers, rows=()):
    barrier = pltpu.get_barrier_semaphore()
    for peer in peers:
        pl.semaphore_signal(barrier, inc=1, device_id={"col": peer}, device_id_type=MESH)
    for peer in rows:
        pl.semaphore_signal(barrier, inc=1, device_id={"row": peer}, device_id_type=MESH)
    pl.semaphore_wait(barrier, len(peers) + len(rows))


def row_peers():
    n = lax.axis_size("row")
    me = lax.axis_index("row")
    steps = sorted(range(1, n), key=lambda step: min(step, n - step))
    return me, tuple(lax.rem(me + step, n) for step in steps), tuple(
        lax.rem(me + n - step, n) for step in steps
    )


def start_rows(pairs, send, recv, local):
    me, peers, sources = row_peers()
    copies = []
    for i, (weight, whole) in enumerate(pairs):
        for j, peer in enumerate(peers):
            c = pltpu.make_async_remote_copy(
                src_ref=weight, dst_ref=whole.at[me],
                send_sem=send.at[i, j], recv_sem=recv.at[i, j],
                device_id={"row": peer}, device_id_type=MESH,
            )
            c.start()
            copies.append(c)
        pltpu.make_async_copy(weight, whole.at[me], local.at[i]).start()


def finish_rows(pairs, send, recv, local):
    me, peers, sources = row_peers()
    for i, (weight, whole) in enumerate(pairs):
        for j, peer in enumerate(peers):
            c = lambda slot: pltpu.make_async_remote_copy(
                src_ref=weight, dst_ref=whole.at[slot],
                send_sem=send.at[i, j], recv_sem=recv.at[i, j],
                device_id={"row": peer}, device_id_type=MESH,
            )
            c(sources[j]).wait_recv()
            c(me).wait_send()
        pltpu.make_async_copy(weight, whole.at[me], local.at[i]).wait()


def neighbours():
    me = lax.axis_index("col")
    core, x, y = me % 2, (me // 2) % 2, me // 4
    place = lambda y, x, core: y * 4 + x * 2 + core
    return (
        me,
        place(y, x, 1 - core),
        place(y, 1 - x, core),
        place(1 - y, x, core),
        place(1 - y, 1 - x, core),
    )


def gather_kernel(count, x_ref, *refs):
    weights, o_ref, wholes = refs[:count], refs[count], refs[count + 1 : 2 * count + 1]
    send, recv, local_sem, wsend, wrecv, wlocal = refs[2 * count + 1 :]
    pairs = tuple(zip(weights, wholes))
    rows = x_ref.shape[0]
    half = rows // 2
    me, mate, xn, yn, dn = neighbours()
    greet((mate, xn, yn), row_peers()[1])

    def part(block, h):
        return o_ref.at[pl.ds(pl.multiple_of(block * rows + h * half, half), half)]

    def copy(i, src, block, h, to):
        return pltpu.make_async_remote_copy(
            src_ref=src, dst_ref=part(block, h), send_sem=send.at[i], recv_sem=recv.at[i],
            device_id={"col": to}, device_id_type=MESH,
        )

    def own(h):
        return x_ref.at[pl.ds(h * half, half)]

    def arrived(i, block, h):
        copy(i, own(0), block, h, mate).wait_recv()

    started = []

    def go(c):
        c.start()
        started.append(c)

    go(copy(0, own(0), me, 0, xn))
    go(copy(1, own(1), me, 1, yn))
    go(copy(2, own(1), me, 1, xn))
    go(copy(3, own(0), me, 0, yn))
    go(copy(6, own(0), me, 0, mate))
    go(copy(7, own(1), me, 1, mate))
    here = pltpu.make_async_copy(
        x_ref, o_ref.at[pl.ds(pl.multiple_of(me * rows, rows), rows)], local_sem
    )
    here.start()
    start_rows(pairs, wsend, wrecv, wlocal)
    arrived(0, xn, 0)
    go(copy(4, part(xn, 0), xn, 0, yn))
    go(copy(8, part(xn, 0), xn, 0, mate))
    arrived(1, yn, 1)
    go(copy(5, part(yn, 1), yn, 1, xn))
    go(copy(9, part(yn, 1), yn, 1, mate))
    arrived(2, xn, 1)
    go(copy(10, part(xn, 1), xn, 1, mate))
    arrived(3, yn, 0)
    go(copy(11, part(yn, 0), yn, 0, mate))
    arrived(4, dn, 0)
    go(copy(12, part(dn, 0), dn, 0, mate))
    arrived(5, dn, 1)
    go(copy(13, part(dn, 1), dn, 1, mate))
    across = lambda block: block + mate - me
    for i, block, h in (
        (6, me, 0), (7, me, 1), (8, xn, 0), (9, yn, 1),
        (10, xn, 1), (11, yn, 0), (12, dn, 0), (13, dn, 1),
    ):
        arrived(i, across(block), h)
    for c in started:
        c.wait_send()
    here.wait()
    finish_rows(pairs, wsend, wrecv, wlocal)


def row_semaphores(count):
    peers = max(lax.axis_size("row") - 1, 1)
    return [
        pltpu.SemaphoreType.DMA((count, peers)),
        pltpu.SemaphoreType.DMA((count, peers)),
        pltpu.SemaphoreType.DMA((count,)),
    ]


def whole_shapes(weights):
    n = lax.axis_size("row")
    return [jax.ShapeDtypeStruct((n, *w.shape), w.dtype) for w in weights]


def gather_col(x, weights, collective_id):
    n = lax.axis_size("col")
    rows, width = x.shape
    vmem = pl.BlockSpec(memory_space=pltpu.VMEM)
    return pl.pallas_call(
        functools.partial(gather_kernel, len(weights)),
        out_shape=[jax.ShapeDtypeStruct((n * rows, width), x.dtype), *whole_shapes(weights)],
        in_specs=[vmem] * (1 + len(weights)),
        out_specs=[vmem] * (1 + len(weights)),
        scratch_shapes=[
            pltpu.SemaphoreType.DMA((14,)),
            pltpu.SemaphoreType.DMA((14,)),
            pltpu.SemaphoreType.DMA,
            *row_semaphores(len(weights)),
        ],
        compiler_params=pltpu.CompilerParams(
            collective_id=collective_id, has_side_effects=True, vmem_limit_bytes=32 << 20
        ),
        cost_estimate=pl.CostEstimate(
            flops=10**10, bytes_accessed=2 * n * rows * width, transcendentals=0
        ),
        name="gather_col",
    )(x, *weights)


def scatter_kernel(x_ref, o_ref, mated, sums, relay, landed, send, recv):
    rows = o_ref.shape[0]
    half = rows // 2
    me, mate, xn, yn, dn = neighbours()
    greet((mate, xn, yn))
    shift = mate - me
    targets = (dn, xn, yn, me)

    def copy(i, src, dst, to):
        return pltpu.make_async_remote_copy(
            src_ref=src, dst_ref=dst, send_sem=send.at[i], recv_sem=recv.at[i],
            device_id={"col": to}, device_id_type=MESH,
        )

    def block(j):
        return pl.ds(pl.multiple_of(j * rows, rows), rows)

    started = []

    def go(c):
        c.start()
        started.append(c)

    for k, target in enumerate(targets):
        go(copy(k, x_ref.at[block(target + shift)], mated.at[k], mate))

    def mine(k, h):
        rows_h = pl.ds(pl.multiple_of(targets[k] * rows + h * half, half), half)
        return x_ref[rows_h, :].astype(jnp.float32) + mated[k, pl.ds(h * half, half), :].astype(
            jnp.float32
        )

    def put(k, h, value):
        sums[k, pl.ds(h * half, half), :] = value.astype(jnp.bfloat16)

    def of(ref, k, h):
        return ref.at[k, pl.ds(h * half, half)]

    started[0].wait_recv()
    put(0, 0, mine(0, 0))
    go(copy(4, of(sums, 0, 0), relay.at[0], xn))
    put(0, 1, mine(0, 1))
    go(copy(5, of(sums, 0, 1), relay.at[1], yn))
    started[1].wait_recv()
    put(1, 0, mine(1, 0))
    go(copy(6, of(sums, 1, 0), of(landed, 0, 0), xn))
    started[2].wait_recv()
    put(2, 1, mine(2, 1))
    go(copy(7, of(sums, 2, 1), of(landed, 1, 1), yn))
    started[4].wait_recv()
    put(2, 0, mine(2, 0) + relay[0].astype(jnp.float32))
    go(copy(8, of(sums, 2, 0), of(landed, 1, 0), yn))
    started[5].wait_recv()
    put(1, 1, mine(1, 1) + relay[1].astype(jnp.float32))
    go(copy(9, of(sums, 1, 1), of(landed, 0, 1), xn))
    started[3].wait_recv()
    for i in (6, 7, 8, 9):
        started[i].wait_recv()
    for h in (0, 1):
        lines = pl.ds(h * half, half)
        o_ref[lines, :] = (
            mine(3, h)
            + landed[0, lines, :].astype(jnp.float32)
            + landed[1, lines, :].astype(jnp.float32)
        )
    for c in started:
        c.wait_send()


def scatter_col(x, collective_id):
    n = lax.axis_size("col")
    rows, width = x.shape[0] // n, x.shape[1]
    if n != 8 or rows % 32:
        return lax.psum_scatter(x, "col", scatter_dimension=0, tiled=True).astype(jnp.float32)
    return pl.pallas_call(
        scatter_kernel,
        out_shape=jax.ShapeDtypeStruct((rows, width), jnp.float32),
        in_specs=[pl.BlockSpec(memory_space=pltpu.VMEM)],
        out_specs=pl.BlockSpec(memory_space=pltpu.VMEM),
        scratch_shapes=[
            pltpu.VMEM((4, rows, width), x.dtype),
            pltpu.VMEM((3, rows, width), x.dtype),
            pltpu.VMEM((2, rows // 2, width), x.dtype),
            pltpu.VMEM((2, rows, width), x.dtype),
            pltpu.SemaphoreType.DMA((10,)),
            pltpu.SemaphoreType.DMA((10,)),
        ],
        compiler_params=pltpu.CompilerParams(
            collective_id=collective_id, has_side_effects=True, vmem_limit_bytes=32 << 20
        ),
        cost_estimate=pl.CostEstimate(
            flops=10**10, bytes_accessed=2 * n * rows * width, transcendentals=0
        ),
        name="scatter_col",
    )(x)


def norm_local(values, gain, bias):
    mean = jnp.mean(values, axis=-1, keepdims=True)
    centred = values - mean
    var = jnp.mean(centred * centred, axis=-1, keepdims=True)
    return centred * lax.rsqrt(var + 1e-06) * gain.astype(jnp.float32) + bias.astype(jnp.float32)


def attend_block(heads, size, padded, query_of, qkv_ref):
    outs = []
    for head in range(heads):
        base = head * 3 * padded
        query = query_of(base)
        keys = qkv_ref[:, base + padded : base + 2 * padded]
        values = qkv_ref[:, base + 2 * padded : base + 3 * padded]
        scores = lax.dot_general(
            query, keys, (((1,), (1,)), ((), ())), preferred_element_type=jnp.float32
        )
        top = jnp.max(scores, axis=-1, keepdims=True)
        expo = jnp.exp2(scores - top).astype(jnp.bfloat16)
        mixed = jnp.dot(expo, values, preferred_element_type=jnp.float32)
        outs.append(mixed[:, :size] / mixed[:, size : size + 1])
    return jnp.concatenate(outs, axis=1)


def attend_kernel(
    heads, size, padded, block, qkv_ref, proj_ref, fc_ref, o_ref, panel_ref, whole_ref,
    send, recv, local_sem, wsend, wrecv, wlocal,
):
    me, mate, xn, yn, dn = neighbours()
    across = mate - me
    greet((mate, xn, yn, dn), row_peers()[1])
    pairs = ((fc_ref, whole_ref),)

    def copy(i, src, slot, to):
        return pltpu.make_async_remote_copy(
            src_ref=src, dst_ref=panel_ref.at[slot], send_sem=send.at[i], recv_sem=recv.at[i],
            device_id={"col": to}, device_id_type=MESH,
        )

    started = [copy(i, proj_ref, me, to) for i, to in enumerate((dn, xn, yn, mate))]
    for c in started:
        c.start()
    here = pltpu.make_async_copy(proj_ref, panel_ref.at[me], local_sem)
    here.start()
    start_rows(pairs, wsend, wrecv, wlocal)

    def step(i, carry):
        rows = pl.ds(pl.multiple_of(i * block, block), block)
        out = attend_block(
            heads, size, padded, lambda base: qkv_ref[rows, base : base + padded], qkv_ref
        )
        o_ref[rows, :] = out.astype(o_ref.dtype)
        return carry

    lax.fori_loop(0, qkv_ref.shape[0] // block, step, 0)

    for i, source in ((1, xn), (2, yn), (0, dn)):
        copy(i, proj_ref, source, mate).wait_recv()
        c = copy(4 + i, panel_ref.at[source], source, mate)
        c.start()
        started.append(c)
    copy(3, proj_ref, mate, mate).wait_recv()
    for i, source in ((1, xn), (2, yn), (0, dn)):
        copy(4 + i, proj_ref, source + across, mate).wait_recv()
    for c in started:
        c.wait_send()
    here.wait()
    finish_rows(pairs, wsend, wrecv, wlocal)


def attend(qkv, proj, weight, heads, size, padded, collective_id):
    length, width = qkv.shape
    block = min(256, length)
    vmem = pl.BlockSpec(memory_space=pltpu.VMEM)
    return pl.pallas_call(
        functools.partial(attend_kernel, heads, size, padded, block),
        in_specs=[vmem] * 3,
        out_specs=[vmem] * 3,
        out_shape=[
            jax.ShapeDtypeStruct((length, heads * size), jnp.bfloat16),
            jax.ShapeDtypeStruct((lax.axis_size("col"), *proj.shape), proj.dtype),
            *whole_shapes([weight]),
        ],
        scratch_shapes=[
            pltpu.SemaphoreType.DMA((7,)),
            pltpu.SemaphoreType.DMA((7,)),
            pltpu.SemaphoreType.DMA,
            *row_semaphores(1),
        ],
        compiler_params=pltpu.CompilerParams(
            collective_id=collective_id, has_side_effects=True, vmem_limit_bytes=48 << 20
        ),
        cost_estimate=pl.CostEstimate(
            flops=4 * heads * length * length * padded * 8,
            bytes_accessed=4 * length * width,
            transcendentals=heads * length * length,
        ),
        name="attend",
    )(qkv, proj, weight)


def plain_attend_kernel(heads, size, padded, q_ref, qkv_ref, o_ref):
    out = attend_block(
        heads, size, padded, lambda base: q_ref[:, base : base + padded], qkv_ref
    )
    o_ref[...] = out.astype(o_ref.dtype)


def plain_attend(qkv, heads, size, padded):
    length, width = qkv.shape
    block = min(256, length)
    return pl.pallas_call(
        functools.partial(plain_attend_kernel, heads, size, padded),
        grid=(length // block,),
        in_specs=[
            pl.BlockSpec((block, width), lambda i: (i, 0)),
            pl.BlockSpec((length, width), lambda i: (0, 0)),
        ],
        out_specs=pl.BlockSpec((block, heads * size), lambda i: (i, 0)),
        out_shape=jax.ShapeDtypeStruct((length, heads * size), jnp.bfloat16),
        compiler_params=pltpu.CompilerParams(vmem_limit_bytes=40 << 20),
        name="attend",
    )(qkv, qkv)


def project_back(left, right):
    return lax.dot_general(
        left, right, (((1,), (1,)), ((), ())), preferred_element_type=jnp.float32
    )


def local(
    tokens_in,
    ln1_gain,
    ln1_bias,
    qkv_weight,
    qkv_bias,
    proj_weight,
    proj_bias,
    ln2_gain,
    ln2_bias,
    fc1_weight,
    fc1_bias,
    fc2_weight,
    fc2_bias,
):
    local_heads = HEADS // lax.axis_size("col")
    own_rows, features = tokens_in.shape
    size = qkv_weight.shape[1] // (3 * local_heads)
    padded = -(-(size + 1) // LANES) * LANES
    inputs = tokens_in.astype(jnp.float32)
    routed = lax.axis_size("col") == 8 and own_rows % 32 == 0
    everyone = functools.partial(lax.all_gather, tiled=True)
    fc1_shift = fc1_bias.astype(jnp.float32)

    ln1 = norm_local(inputs, ln1_gain, ln1_bias).astype(jnp.bfloat16)
    if routed:
        tokens, qkv_full, proj_full = gather_col(ln1, (qkv_weight, proj_weight), 0)
        qkv_full = qkv_full.reshape(features, -1)
        proj_full = proj_full.swapaxes(0, 1).reshape(-1, features)
    else:
        tokens = everyone(ln1, "col", axis=0)
        qkv_full = everyone(qkv_weight, "row", axis=0)
        proj_full = everyone(proj_weight, "row", axis=1)

    spare = padded - size
    qkv_wide = jnp.pad(
        qkv_full.reshape(features, local_heads, 3, size), ((0, 0), (0, 0), (0, 0), (0, spare))
    ).reshape(features, local_heads * 3 * padded)
    shift = jnp.pad(
        qkv_bias.astype(jnp.float32).reshape(local_heads, 3, size), ((0, 0), (0, 0), (0, spare))
    )
    shift = shift.at[:, 2, size].set(1.0).reshape(-1)
    scale = jnp.ones((local_heads, 3, padded), jnp.float32)
    scale = scale.at[:, 0].set(1.4426950408889634 / size**0.5).reshape(-1)

    product = jnp.dot(tokens, qkv_wide, preferred_element_type=jnp.float32)
    qkv = ((product + shift) * scale).astype(jnp.bfloat16)
    if routed:
        attn, proj_whole, fc1_full = attend(
            qkv, proj_full, fc1_weight, local_heads, size, padded, 3
        )
        proj_whole = proj_whole.reshape(-1, features)
        fc1_full = fc1_full.reshape(features, -1)
    else:
        attn = plain_attend(qkv, local_heads, size, padded)
        proj_whole = everyone(proj_full, "col", axis=0)
        fc1_full = everyone(fc1_weight, "row", axis=0)
    own_heads = lax.all_to_all(attn, "col", split_axis=0, concat_axis=1, tiled=True)
    attn_sum = jnp.dot(own_heads, proj_whole, preferred_element_type=jnp.float32)
    resid = inputs + attn_sum + proj_bias.astype(jnp.float32)
    ln2 = norm_local(resid, ln2_gain, ln2_bias).astype(jnp.bfloat16)
    if routed:
        tokens, fc2_full = gather_col(ln2, (fc2_weight,), 1)
        fc2_full = fc2_full.reshape(features, -1)
    else:
        tokens = everyone(ln2, "col", axis=0)
        fc2_full = everyone(fc2_weight, "row", axis=0)
    product = jnp.dot(tokens, fc1_full, preferred_element_type=jnp.float32) + fc1_shift
    hidden = jax.nn.gelu(product, approximate=False).astype(jnp.bfloat16)
    mlp_sum = scatter_col(project_back(hidden, fc2_full).astype(jnp.bfloat16), 2)
    result = resid + mlp_sum + fc2_bias.astype(jnp.float32)
    return result.astype(jnp.bfloat16)


def solution(mesh):
    in_specs = (
        P(("row", "col"), None),
        P(),
        P(),
        P("row", "col"),
        P("col"),
        P("col", "row"),
        P(),
        P(),
        P(),
        P("row", "col"),
        P("col"),
        P("row", "col"),
        P(),
    )
    out_specs = P(("row", "col"), None)
    return jax.shard_map(local, mesh=mesh, in_specs=in_specs, out_specs=out_specs, check_vma=False)
```
